256 devices in a mesh: pq: 8 (over z_hi, x), rs: 32 (over y, z_lo, core).
Axes of the slice: x: 4, y: 4, z: 8 (z_hi: 2, z_lo: 4; z = z_hi * 4 + z_lo), core: 2. Of those that a mesh axis runs over, the one named last changes fastest.
Arguments:
- integrals: bfloat16 [512, 1152, 1152], P('pq', 'rs'), may hold values from -6 to 6
- coeff: bfloat16 [1152, 896], P('rs', 'pq'), may hold values from -0.1875 to 0.1875
Outputs:
- half_mo: bfloat16 [512, 896, 896], P('pq', 'rs')
The draws below stay inside these ranges and needn't reach their ends.
All inputs are finite; a program needn't handle non-finite values.
Results may differ from the reference program's by a relative error of at most 0.0049.
Values may be sent and summed in bfloat16 or wider, within the bound.
No kernel may reach another device: no remote copies, remote signals or barrier semaphores. Data moves between devices by JAX's collectives and lax.ppermute only.
A program may use at most 128 MiB of HBM per device.

```python
import jax
import jax.numpy as jnp
from jax import lax

NBASIS = 1152
NORB = 896
PAIRS = 512


def block_scale(own_key, dims, split, smallest, top_value):
    factor_of, own = 1.0, jax.random.fold_in(own_key, 6)
    for dim, parts in split:
        steps = jnp.exp(jax.random.uniform(jax.random.fold_in(own, dim), (parts,), jnp.float32, smallest / len(split), top_value / len(split)))
        factor_of = factor_of * jnp.repeat(steps, dims[dim] // parts).reshape([-1 if axis == dim else 1 for axis in range(len(dims))])
    return factor_of


def noise(own_key, shape, width, bound, cuts=(), kind=jnp.bfloat16):
    drawn = width * jax.random.normal(own_key, shape, jnp.float32)
    if cuts:
        drawn = drawn * block_scale(own_key, shape, cuts, -0.22, 0.18)
    return jnp.clip(drawn, -bound, bound).astype(kind)


def setup_inputs(seed: int = 0) -> dict:
    splits = jax.random.split(jax.random.key(seed), 3)
    return {
        "integrals": noise(splits[0], (PAIRS, NBASIS, NBASIS), 1.0, 6.0, ((0, 8), (1, 32))),
        "coeff": noise(splits[1], (NBASIS, NORB), NBASIS ** -0.5, 0.1875, ((0, 32), (1, 8))),
    }


def reference(integrals, coeff):
    pairs = integrals.shape[0]
    flat = integrals.reshape(pairs * NBASIS, NBASIS)
    first = jnp.dot(flat, coeff, preferred_element_type=jnp.float32).astype(jnp.bfloat16)
    first = first.reshape(pairs, NBASIS, NORB)

    def one_row(block):
        return jnp.dot(block.T, coeff, preferred_element_type=jnp.float32).astype(jnp.bfloat16)

    return lax.map(one_row, first)
```

```python
import jax
import jax.numpy as jnp
from jax import lax
from jax.experimental import pallas as pl
from jax.experimental.pallas import tpu as pltpu
from jax.sharding import PartitionSpec as P


NBASIS = 1152
NORB = 896
SIZES = (8, 16, 4)
BOTH = ("pq", "rs")


def place(z_hi, x, y, z_lo, core):
    return (z_hi * 4 + x) * 32 + y * 8 + z_lo * 2 + core


ALONG_Z = [
    [place(h, x, y, z, c) for h in range(2) for z in range(4) for c in range(2)]
    for x in range(4)
    for y in range(4)
]
ACROSS = [
    [place(h, x, y, z, c) for x in range(4) for y in range(4)]
    for h in range(2)
    for z in range(4)
    for c in range(2)
]


def from_group(array, groups):
    copies = jnp.broadcast_to(array[None], (len(groups[0]), *array.shape))
    return lax.all_to_all(copies, BOTH, 0, 0, tiled=True, axis_index_groups=groups)


def one_hot(match):
    return match.astype(jnp.bfloat16)


def pick(array, chosen):
    return jnp.dot(array, chosen, preferred_element_type=jnp.float32).astype(jnp.bfloat16)


def join_kernel(own_ref, a_ref, b_ref, c_ref, d_ref, out_ref, *, width):
    total = jnp.zeros(out_ref.shape, jnp.float32)
    for step, ref in enumerate((a_ref, b_ref, c_ref, d_ref)):
        for h in range(2):
            owner = h * 4 + (own_ref[0] ^ step)
            inside = lax.broadcasted_iota(jnp.int32, (128, NORB), 0)
            column = lax.broadcasted_iota(jnp.int32, (128, NORB), 1)
            keep = (inside < width) & (column == owner * width + inside)
            chosen = jnp.where(keep, 1.0, 0.0).astype(jnp.bfloat16)
            total += jnp.dot(ref[h], chosen, preferred_element_type=jnp.float32)
    out_ref[...] = total.astype(out_ref.dtype)


def join(slabs, x, width):
    block = 384
    return pl.pallas_call(
        lambda *refs: join_kernel(*refs, width=width),
        grid=(NBASIS // block,),
        in_specs=[pl.BlockSpec(memory_space=pltpu.SMEM)]
        + [pl.BlockSpec((2, block, 128), lambda i: (0, i, 0))] * 4,
        out_specs=pl.BlockSpec((block, NORB), lambda i: (i, 0)),
        out_shape=jax.ShapeDtypeStruct((NBASIS, NORB), jnp.bfloat16),
        name="join",
    )(x.reshape(1), *slabs)


def leave(part, flat, count, lanes):
    first = jnp.einsum("sc,ms->cm", part, flat, preferred_element_type=jnp.float32)
    return first.astype(jnp.bfloat16).reshape(count, -1, lanes)


def on_device(integrals, coeff):
    pairs, rows, _ = integrals.shape
    width = coeff.shape[1]
    count = lax.axis_size("rs")
    mine = NORB // count
    x = lax.axis_index("pq") % 4
    y = lax.axis_index("rs") // 8
    flat = integrals.transpose(1, 0, 2).reshape(rows * pairs, NBASIS)

    strip = from_group(jnp.pad(coeff, ((0, 0), (0, 128 - width))), ALONG_Z)
    strip = strip.reshape(2, 8 * rows, 128)

    size = SIZES[0]
    inner, outer = lax.broadcasted_iota(jnp.int32, (128, 4 * size), 0), lax.broadcasted_iota(
        jnp.int32, (128, 4 * size), 1
    )
    chosen = one_hot(inner == outer // size * mine + outer % size)
    early = pick(strip.reshape(16 * rows, 128), chosen)
    early_sent = early.reshape(-1, 8, 128)
    early = from_group(early_sent, ACROSS)
    early = early.reshape(4, 4, 2, 8 * rows, 4 * size).transpose(1, 3, 2, 0, 4)
    early = early.reshape(NBASIS, count * size)

    first = leave(early, flat, count, rows * pairs)

    strip, _ = lax.optimization_barrier((strip, early_sent))
    stack = [strip]
    for step in (1, 2, 3):
        stack.append(
            lax.ppermute(strip, "rs", [(j, (j // 8 ^ step) * 8 + j % 8) for j in range(32)])
        )
    low, high = y % 2 == 1, y // 2 == 1
    stack = [jnp.where(low, stack[i ^ 1], stack[i]) for i in range(4)]
    stack = jnp.stack([jnp.where(high, stack[i ^ 2], stack[i]) for i in range(4)], 1)
    slabs = [stack.reshape(2, NBASIS, 128)]
    for step in (1, 2, 3):
        slabs.append(lax.ppermute(slabs[0], "pq", [(i, i & 4 | (i & 3) ^ step) for i in range(8)]))
    panel = join(slabs, x, width)
    by_row = panel.reshape(count, rows, NORB)

    outs = []
    lo = 0
    for size in SIZES:
        if lo:
            target = lax.broadcasted_iota(jnp.int32, (NORB, count * size), 1)
            source = lax.broadcasted_iota(jnp.int32, (NORB, count * size), 0)
            part = pick(panel, one_hot(source == target // size * mine + lo + target % size))
            part, _ = lax.optimization_barrier((part, first))
            first = leave(part, flat, count, rows * pairs)
        lo += size
        got = lax.all_to_all(first, "rs", 0, 0, tiled=True)
        got = got.reshape(count, size, rows, pairs)
        outs.append(
            jnp.einsum("jlrp,jrk->lpk", got, by_row, preferred_element_type=jnp.float32).astype(
                jnp.bfloat16
            )
        )
    return jnp.concatenate(outs, 0).transpose(1, 0, 2)


def solution(mesh):
    placed = (P("pq", "rs", None), P("rs", "pq"))
    return jax.shard_map(
        on_device, mesh=mesh, in_specs=placed, out_specs=P("pq", "rs", None), check_vma=False
    )
```

```python
import functools

import jax
import jax.numpy as jnp
from jax import lax
from jax.experimental import pallas as pl
from jax.experimental.pallas import tpu as pltpu
from jax.sharding import PartitionSpec as P


NBASIS = 1152
NORB = 896
MINE = 28
WIDTH = 112
ROWS = 36
PAIRS = 64
COUNT = 32
LANES = ROWS * PAIRS
NEAR, FAR, LAST = 8, 16, 4
BOTH = ("pq", "rs")


def place(z_hi, x, y, z_lo, core):
    return (z_hi * 4 + x) * 32 + y * 8 + z_lo * 2 + core


ALONG_Z = [
    [place(h, x, y, z, c) for h in range(2) for z in range(4) for c in range(2)]
    for x in range(4)
    for y in range(4)
]
ACROSS = [
    [place(h, x, y, z, c) for x in range(4) for y in range(4)]
    for h in range(2)
    for z in range(4)
    for c in range(2)
]


def from_group(array, groups):
    copies = jnp.broadcast_to(array[None], (len(groups[0]), *array.shape))
    return lax.all_to_all(copies, BOTH, 0, 0, tiled=True, axis_index_groups=groups)


def iota(shape, dim):
    return lax.broadcasted_iota(jnp.int32, shape, dim)


def one_hot(match):
    return jnp.where(match, 1.0, 0.0).astype(jnp.bfloat16)


def pick(array, chosen):
    return jnp.dot(array, chosen, preferred_element_type=jnp.float32).astype(jnp.bfloat16)


def join_kernel(own_ref, a_ref, b_ref, c_ref, d_ref, out_ref):
    total = jnp.zeros(out_ref.shape, jnp.float32)
    for step, ref in enumerate((a_ref, b_ref, c_ref, d_ref)):
        for h in range(2):
            owner = h * 4 + (own_ref[0] ^ step)
            shape = (WIDTH, NORB)
            chosen = one_hot(iota(shape, 1) == owner * WIDTH + iota(shape, 0))
            total += jnp.dot(ref[h], chosen, preferred_element_type=jnp.float32)
    out_ref[...] = total.astype(out_ref.dtype)


def join(slabs, x):
    block = 576
    return pl.pallas_call(
        join_kernel,
        grid=(NBASIS // block,),
        in_specs=[pl.BlockSpec(memory_space=pltpu.SMEM)]
        + [pl.BlockSpec((2, block, WIDTH), lambda i: (0, i, 0))] * 4,
        out_specs=pl.BlockSpec((block, NORB), lambda i: (i, 0)),
        out_shape=jax.ShapeDtypeStruct((NBASIS, NORB), jnp.bfloat16),
        name="join",
    )(x.reshape(1), *slabs)


def early_kernel(own_ref, columns_ref, low_ref, high_ref, near_ref, *rest):
    *last_refs, part, turned = rest
    step = pl.program_id(0)
    edge = COUNT * NEAR

    @pl.when(step == 0)
    def _():
        for x in range(4):
            for h in range(2):
                for size, top, base in ((NEAR, 0, 0), (LAST, 4 * NEAR, edge)):
                    lines = 4 * size
                    strips = [
                        columns_ref[x * 4 + y, pl.ds(top, lines), pl.ds(h * 288, 288)]
                        for y in range(4)
                    ]
                    part[pl.ds(base + (h * 4 + x) * lines, lines), :] = jnp.concatenate(strips, 1)
        shape = (COUNT * LAST, COUNT * LAST)
        to, come = iota(shape, 0), iota(shape, 1)
        d = to // LAST
        d = (d & 6) << 2 | (d & 24) >> 2 | d & 1
        swap = one_hot((come // LAST == (d ^ own_ref[0])) & (come % LAST == to % LAST))
        last = jnp.dot(swap, part[edge:, :], preferred_element_type=jnp.float32)
        part[edge:, :] = last.astype(part.dtype)
        turned[...] = part[...].T

    lanes = pl.ds(pl.multiple_of(step * low_ref.shape[0], 128), low_ref.shape[0])
    lasts = []
    for half, ref in enumerate((low_ref, high_ref)):
        first = jnp.dot(ref[...], turned[...], preferred_element_type=jnp.float32)
        first = first.astype(jnp.bfloat16).T
        block = first.shape[1]
        at = pl.multiple_of(half * (LANES // 2) + step * block, 128)
        near_ref[:, :, pl.ds(at, block)] = first[:edge].reshape(COUNT, NEAR, block)
        lasts.append(first[edge:].astype(jnp.float32).reshape(COUNT, LAST, block))
    lasts = jnp.concatenate(lasts, 1).astype(jnp.bfloat16)
    for step, ref in enumerate(last_refs):
        ref[:, :, lanes] = lasts[8 * step : 8 * step + 8]


def early_first(columns, flat, own):
    block = 384
    steps = LANES // 2 // block
    return pl.pallas_call(
        early_kernel,
        grid=(steps,),
        in_specs=[
            pl.BlockSpec(memory_space=pltpu.SMEM),
            pl.BlockSpec(columns.shape, lambda i: (0, 0, 0)),
            pl.BlockSpec((block, NBASIS), lambda i: (i, 0)),
            pl.BlockSpec((block, NBASIS), lambda i: (i + steps, 0)),
        ],
        out_specs=[
            pl.BlockSpec((COUNT, NEAR, LANES), lambda i: (0, 0, 0)),
        ]
        + [pl.BlockSpec((8, 2 * LAST, LANES // 2), lambda i: (0, 0, 0))] * 4,
        out_shape=[
            jax.ShapeDtypeStruct((COUNT, NEAR, LANES), jnp.bfloat16),
        ]
        + [jax.ShapeDtypeStruct((8, 2 * LAST, LANES // 2), jnp.bfloat16)] * 4,
        scratch_shapes=[
            pltpu.VMEM((COUNT * (NEAR + LAST), NBASIS), jnp.bfloat16),
            pltpu.VMEM((NBASIS, COUNT * (NEAR + LAST)), jnp.bfloat16),
        ],
        name="early_first",
    )(own.reshape(1), columns, flat, flat)


def leave(part, flat):
    first = jnp.einsum("sc,ms->cm", part, flat, preferred_element_type=jnp.float32)
    return first.astype(jnp.bfloat16).reshape(COUNT, -1, LANES)


def slot_of(r, j):
    tile, odd = r // 2, r % 2
    return jnp.where(
        tile < 16, odd * 512 + tile * 32 + j, 1024 + odd * 64 + (tile - 16) * 32 + j
    )


def second_kernel(got_ref, panel_ref, *rest, halves):
    out_ref, wide, lhs = rest[-3:]
    count, lines, lanes = got_ref.shape
    mine = lines // halves
    tiles = lanes // 128
    for tile in range(tiles):
        piece = got_ref[:, :, pl.ds(tile * 128, 128)].astype(jnp.float32)
        wide[pl.ds(tile * count * lines, count * lines), :] = piece.reshape(count * lines, 128)
    for l in range(mine):
        rows = pl.ds(l * PAIRS, PAIRS)
        for start in range(0, 18, 4):
            parts = []
            for tile in range(start, min(start + 4, 18)):
                half, at = tile // tiles, tile % tiles
                top = at * count * lines + half * mine + l
                parts.append(wide[pl.ds(top, count, stride=lines), :])
            turned = jnp.concatenate(parts, 0).astype(jnp.bfloat16).T
            if len(parts) == 4:
                lhs[rows, pl.ds(start * 32, 128)] = turned[:PAIRS]
                lhs[rows, pl.ds(512 + start * 32, 128)] = turned[PAIRS:]
            else:
                lhs[rows, pl.ds(1024, 128)] = jnp.concatenate([turned[:PAIRS], turned[PAIRS:]], 1)
    product = jnp.dot(lhs[...], panel_ref[...], preferred_element_type=jnp.float32)
    out_ref[...] = product.astype(out_ref.dtype).reshape(out_ref.shape)


def second(got, ordered, into, lo, halves=1):
    count, lines, lanes = got.shape
    block = 8 // halves
    specs = [
        pl.BlockSpec((count, 8, lanes), lambda i: (0, i, 0)),
        pl.BlockSpec(ordered.shape, lambda i: (0, 0)),
    ]
    operands = [got, ordered]
    aliases = {}
    if into is not None:
        specs.append(pl.BlockSpec(memory_space=pl.ANY))
        operands.append(into)
        aliases = {2: 0}
    return pl.pallas_call(
        functools.partial(second_kernel, halves=halves),
        grid=(lines // 8,),
        in_specs=specs,
        out_specs=pl.BlockSpec((block, PAIRS, NORB), lambda i: (lo // block + i, 0, 0)),
        out_shape=jax.ShapeDtypeStruct((MINE, PAIRS, NORB), jnp.bfloat16),
        scratch_shapes=[
            pltpu.VMEM((count * 8 * lanes // 128, 128), jnp.float32),
            pltpu.VMEM((block * PAIRS, NBASIS), jnp.bfloat16),
        ],
        input_output_aliases=aliases,
        name="second",
    )(*operands)


def ordering(panel, place_of):
    shape = (NBASIS, NBASIS)
    slot = slot_of(iota(shape, 1) % ROWS, place_of(iota(shape, 1) // ROWS))
    return pick(one_hot(slot == iota(shape, 0)), panel)


def select(chosen, strip):
    columns = jnp.dot(chosen, strip.reshape(-1, WIDTH).T, preferred_element_type=jnp.float32)
    return columns.astype(jnp.bfloat16)


def on_device(integrals, coeff):
    x = lax.axis_index("pq") % 4
    own = lax.axis_index("rs")
    y = own // 8
    flat = integrals.transpose(1, 0, 2).reshape(LANES, NBASIS)

    strip = from_group(coeff, ALONG_Z).reshape(2, 8 * ROWS, WIDTH)

    shape = (4 * (NEAR + LAST), WIDTH)
    row, edge = iota(shape, 0), 4 * NEAR
    wanted = jnp.where(
        row < edge,
        row // NEAR * MINE + row % NEAR,
        (row - edge) // LAST * MINE + NEAR + FAR + (row - edge) % LAST,
    )
    columns = select(one_hot(iota(shape, 1) == wanted), strip)
    early = from_group(columns, ACROSS)
    near, *last = early_first(early, flat, own)

    stack = [strip]
    for step in (1, 2, 3):
        stack.append(lax.ppermute(strip, "rs", [(j, j ^ step * 8) for j in range(COUNT)]))
    low, high = y % 2 == 1, y // 2 == 1
    stack = [jnp.where(low, stack[i ^ 1], stack[i]) for i in range(4)]
    stack = jnp.stack([jnp.where(high, stack[i ^ 2], stack[i]) for i in range(4)], 1)
    slab = stack.reshape(2, NBASIS, WIDTH)
    slabs = [slab]
    for step in (1, 2, 3):
        slabs.append(lax.ppermute(slab, "pq", [(i, i & 4 | (i & 3) ^ step) for i in range(8)]))
    panel = join(slabs, x)

    got_near = lax.all_to_all(near, "rs", 0, 0, tiled=True)

    held = [last[0]]
    for step in (1, 2, 3):
        held.append(
            lax.ppermute(last[step], "rs", [(j, j ^ step * 2) for j in range(COUNT)])
        )
    held = jnp.stack(held, 1)
    got_last = [held[0]]
    for step in range(1, 8):
        got_last.append(
            lax.ppermute(
                held[step],
                "rs",
                [(j, j ^ (step // 2 * 8 + step % 2)) for j in range(COUNT)],
            )
        )
    got_last = jnp.concatenate(got_last, 0)

    shape = (NORB, COUNT * FAR)
    source = iota(shape, 1) // FAR * MINE + NEAR + iota(shape, 1) % FAR
    part = lax.optimization_barrier(pick(panel, one_hot(iota(shape, 0) == source)))
    far = leave(part, flat)
    got_far = lax.all_to_all(far, "rs", 0, 0, tiled=True)

    ordered = ordering(panel, lambda j: j)
    crossed = ordering(panel, lambda j: ((j ^ own) & 24) | ((j ^ own) & 1) << 2 | ((j ^ own) & 6) >> 1)
    out = second(got_near, ordered, None, 0)
    out = second(got_last, crossed, out, NEAR + FAR, halves=2)
    out = second(got_far, ordered, out, NEAR)
    return out.transpose(1, 0, 2)


def solution(mesh):
    placed = (P("pq", "rs", None), P("rs", "pq"))
    return jax.shard_map(
        on_device, mesh=mesh, in_specs=placed, out_specs=P("pq", "rs", None), check_vma=False
    )
```

```python
import functools

import jax
import jax.numpy as jnp
from jax import lax
from jax.experimental import pallas as pl
from jax.experimental.pallas import tpu as pltpu
from jax.sharding import PartitionSpec as P


NBASIS = 1152
NORB = 896
MINE = 28
WIDTH = 112
ROWS = 36
PAIRS = 64
COUNT = 32
LANES = ROWS * PAIRS
SOON, FAR = 2, 5
HALF = LANES // 2
BOTH = ("pq", "rs")


def place(z_hi, x, y, z_lo, core):
    return (z_hi * 4 + x) * 32 + y * 8 + z_lo * 2 + core


ALONG_Z = [
    [place(h, x, y, z, c) for h in range(2) for z in range(4) for c in range(2)]
    for x in range(4)
    for y in range(4)
]


def from_group(array, groups):
    copies = jnp.broadcast_to(array[None], (len(groups[0]), *array.shape))
    return lax.all_to_all(copies, BOTH, 0, 0, tiled=True, axis_index_groups=groups)


def iota(shape, dim):
    return lax.broadcasted_iota(jnp.int32, shape, dim)


def one_hot(match):
    return jnp.where(match, 1.0, 0.0).astype(jnp.bfloat16)


def pick(array, chosen):
    return jnp.dot(array, chosen, preferred_element_type=jnp.float32).astype(jnp.bfloat16)


def spot(d, own):
    return ((d & 6) << 2 | (d & 24) >> 2 | d & 1) ^ own


def first_kernel(
    own_ref, x_ref, a_ref, b_ref, c_ref, d_ref, low_ref, high_ref, *rest, groups, permuted
):
    *near_refs, part, turned = rest
    near_refs, far_refs = (near_refs[:4], ()) if permuted else ((), near_refs)
    block = low_ref.shape[0]

    @pl.when(pl.program_id(0) == 0)
    def _():
        y = own_ref[0] >> 3
        for step, ref in enumerate((a_ref, b_ref, c_ref, d_ref)):
            for h in range(2):
                strips = [ref[y ^ k, :, pl.ds(h * 288, 288)] for k in range(4)]
                rows = jnp.concatenate(strips, 1)
                for group in range(groups):
                    top = group * 128 + (h * 4 + (x_ref[0] ^ step)) * 16
                    part[pl.ds(pl.multiple_of(top, 16), 16), :] = rows[group * 16 : group * 16 + 16]
        shape = (COUNT * 4, COUNT * 4)
        to, come = iota(shape, 0), iota(shape, 1)
        swap = one_hot((come // 4 == spot(to // 4, own_ref[0])) & (come % 4 == to % 4))
        for group in range(groups if permuted else 0):
            at = pl.ds(group * 128, 128)
            moved = jnp.dot(swap, part[at, :], preferred_element_type=jnp.float32)
            part[at, :] = moved.astype(part.dtype)
        turned[...] = part[...].T

    firsts = []
    for ref in (low_ref, high_ref):
        first = jnp.dot(ref[...], turned[...], preferred_element_type=jnp.float32).T
        firsts.append(first.reshape(groups, COUNT, 4, block))
    firsts = jnp.concatenate(firsts, 2).astype(jnp.bfloat16)
    for group in range(groups):
        at = pl.ds(pl.multiple_of(group * HALF + pl.program_id(0) * block, 128), block)
        for step, ref in enumerate(near_refs):
            ref[:, :, at] = firsts[group, 8 * step : 8 * step + 8]
        for ref in far_refs:
            ref[:, :, at] = firsts[group]


def first_product(slabs, flat, own, x, permuted):
    block = 384
    steps = HALF // block
    groups = slabs[0].shape[1] // 16
    shapes = [(8, 8, groups * HALF)] * 4 if permuted else [(COUNT, 8, groups * HALF)]
    whole = lambda shape: pl.BlockSpec(shape, lambda i: (0,) * len(shape))
    shapes.append((groups * 128, NBASIS))
    return pl.pallas_call(
        functools.partial(first_kernel, groups=groups, permuted=permuted),
        grid=(steps,),
        in_specs=[pl.BlockSpec(memory_space=pltpu.SMEM)] * 2
        + [whole(slabs[0].shape)] * 4
        + [
            pl.BlockSpec((block, NBASIS), lambda i: (i, 0)),
            pl.BlockSpec((block, NBASIS), lambda i: (i + steps, 0)),
        ],
        out_specs=[whole(shape) for shape in shapes],
        out_shape=[jax.ShapeDtypeStruct(shape, jnp.bfloat16) for shape in shapes],
        scratch_shapes=[pltpu.VMEM((NBASIS, groups * 128), jnp.bfloat16)],
    )(own.reshape(1), x.reshape(1), *slabs, flat, flat)


def slot_of(r, j):
    tile, odd = r // 2, r % 2
    return jnp.where(
        tile < 16, odd * 512 + tile * 32 + j, 1024 + odd * 64 + (tile - 16) * 32 + j
    )


def second_kernel(got_ref, panel_ref, *rest):
    out_ref, wide, lhs = rest[-3:]
    size = COUNT * 8
    for tile in range(HALF // 128):
        piece = got_ref[:, :, pl.ds(tile * 128, 128)].astype(jnp.float32)
        wide[pl.ds(tile * size, size), :] = piece.reshape(size, 128)
    for l in range(4):
        rows = pl.ds(l * PAIRS, PAIRS)
        for start in range(0, 18, 4):
            parts = []
            for tile in range(start, min(start + 4, 18)):
                top = tile % 9 * size + tile // 9 * 4 + l
                parts.append(wide[pl.ds(top, COUNT, stride=8), :])
            turned = jnp.concatenate(parts, 0).astype(jnp.bfloat16).T
            if len(parts) == 4:
                lhs[rows, pl.ds(start * 32, 128)] = turned[:PAIRS]
                lhs[rows, pl.ds(512 + start * 32, 128)] = turned[PAIRS:]
            else:
                lhs[rows, pl.ds(1024, 128)] = jnp.concatenate([turned[:PAIRS], turned[PAIRS:]], 1)
    product = jnp.dot(lhs[...], panel_ref[...], preferred_element_type=jnp.float32)
    out_ref[...] = product.astype(out_ref.dtype).reshape(out_ref.shape)


def second(got, ordered, into, lo):
    specs = [
        pl.BlockSpec((COUNT, 8, HALF), lambda i: (0, 0, i)),
        pl.BlockSpec(ordered.shape, lambda i: (0, 0)),
    ]
    operands = [got, ordered]
    aliases = {}
    if into is not None:
        specs.append(pl.BlockSpec(memory_space=pl.ANY))
        operands.append(into)
        aliases = {2: 0}
    return pl.pallas_call(
        second_kernel,
        grid=(got.shape[2] // HALF,),
        in_specs=specs,
        out_specs=pl.BlockSpec((4, PAIRS, NORB), lambda i: (lo + i, 0, 0)),
        out_shape=jax.ShapeDtypeStruct((MINE, PAIRS, NORB), jnp.bfloat16),
        scratch_shapes=[
            pltpu.VMEM((COUNT * 8 * HALF // 128, 128), jnp.float32),
            pltpu.VMEM((4 * PAIRS, NBASIS), jnp.bfloat16),
        ],
        input_output_aliases=aliases,
        name="second",
    )(*operands)


def ordering(panel, place_of):
    shape = (NBASIS, NBASIS)
    slot = slot_of(iota(shape, 1) % ROWS, place_of(iota(shape, 1) // ROWS))
    return pick(one_hot(slot == iota(shape, 0)), panel)


def columns_of(first, groups, strip):
    shape = (16 * groups, WIDTH)
    row = iota(shape, 0)
    column = row % 16 // 4 * MINE + (first + row // 16) * 4 + row % 4
    chosen = one_hot(iota(shape, 1) == column)
    rows = jnp.dot(chosen, strip.reshape(-1, WIDTH).T, preferred_element_type=jnp.float32)
    return rows.astype(jnp.bfloat16)


def spread(first):
    held = [first[0]]
    for step in (1, 2, 3):
        held.append(lax.ppermute(first[step], "rs", [(j, j ^ step * 2) for j in range(COUNT)]))
    held = jnp.stack(held, 1)
    got = [held[0]]
    for step in range(1, 8):
        pairs = [(j, j ^ (step // 2 * 8 + step % 2)) for j in range(COUNT)]
        got.append(lax.ppermute(held[step], "rs", pairs))
    return jnp.concatenate(got, 0)


def on_device(integrals, coeff):
    x = lax.axis_index("pq") % 4
    own = lax.axis_index("rs")
    flat = integrals.transpose(1, 0, 2).reshape(LANES, NBASIS)

    strip = from_group(coeff, ALONG_Z).reshape(2, 8 * ROWS, WIDTH)
    columns = columns_of(0, SOON + FAR, strip)
    slab = [columns]
    for step in (1, 2, 3):
        slab.append(lax.ppermute(columns, "rs", [(j, j ^ step * 8) for j in range(COUNT)]))

    def over_x(lo, hi):
        own_slab = jnp.stack([part[lo * 16 : hi * 16] for part in slab])
        slabs = [own_slab]
        for step in (1, 2, 3):
            pairs = [(i, i & 4 | (i & 3) ^ step) for i in range(8)]
            slabs.append(lax.ppermute(own_slab, "pq", pairs))
        return slabs

    early = over_x(0, SOON)
    late = over_x(SOON, SOON + FAR)
    *soon, soon_part = first_product(early, flat, own, x, True)
    far, far_part = first_product(late, flat, own, x, False)

    got_soon = spread(soon)
    got_far = lax.all_to_all(far, "rs", 0, 0, tiled=True)

    far_part, mine = lax.optimization_barrier((far_part, own))
    parts = jnp.concatenate([soon_part, far_part], 0)
    g = iota((NORB, NORB), 0)
    d = g % 128 // 4
    j = jnp.where(g < SOON * 128, spot(d, mine), d)
    put = one_hot(iota((NORB, NORB), 1) == j * MINE + g // 128 * 4 + g % 4)
    panel = jnp.einsum("gs,gk->sk", parts, put, preferred_element_type=jnp.float32)
    panel = panel.astype(jnp.bfloat16)
    ordered = ordering(panel, lambda j: j)
    crossed = ordering(
        panel, lambda j: ((j ^ mine) & 24) | ((j ^ mine) & 1) << 2 | ((j ^ mine) & 6) >> 1
    )
    out = second(got_soon, crossed, None, 0)
    out = second(got_far, ordered, out, SOON)
    return out.transpose(1, 0, 2)


def solution(mesh):
    placed = (P("pq", "rs", None), P("rs", "pq"))
    return jax.shard_map(
        on_device, mesh=mesh, in_specs=placed, out_specs=P("pq", "rs", None), check_vma=False
    )
```

```python
import functools

import jax
import jax.numpy as jnp
from jax import lax
from jax.experimental import pallas as pl
from jax.experimental.pallas import tpu as pltpu
from jax.sharding import PartitionSpec as P


NBASIS = 1152
NORB = 896
MINE = 28
WIDTH = 112
ROWS = 36
PAIRS = 64
COUNT = 32
LANES = ROWS * PAIRS
SOON, FAR = 2, 5
HALF = LANES // 2
ALL_VMEM = 63 * 2**20
BOTH = ("pq", "rs")


def place(z_hi, x, y, z_lo, core):
    return (z_hi * 4 + x) * 32 + y * 8 + z_lo * 2 + core


ALONG_Z = [
    [place(h, x, y, z, c) for h in range(2) for z in range(4) for c in range(2)]
    for x in range(4)
    for y in range(4)
]


def from_group(array, groups):
    copies = jnp.broadcast_to(array[None], (len(groups[0]), *array.shape))
    return lax.all_to_all(copies, BOTH, 0, 0, tiled=True, axis_index_groups=groups)


def iota(shape, dim):
    return lax.broadcasted_iota(jnp.int32, shape, dim)


def one_hot(match):
    return jnp.where(match, 1.0, 0.0).astype(jnp.bfloat16)


def pick(array, chosen):
    return jnp.dot(array, chosen, preferred_element_type=jnp.float32).astype(jnp.bfloat16)


def spot(d, own):
    return ((d & 6) << 2 | (d & 24) >> 2 | d & 1) ^ own


def first_kernel(
    own_ref, x_ref, a_ref, b_ref, c_ref, d_ref, low_ref, high_ref, *rest, groups, permuted
):
    *near_refs, part, turned = rest
    near_refs, far_refs = (near_refs[:4], ()) if permuted else ((), near_refs)
    block = low_ref.shape[0]

    @pl.when(pl.program_id(0) == 0)
    def _():
        y = own_ref[0] >> 3
        for step, ref in enumerate((a_ref, b_ref, c_ref, d_ref)):
            for h in range(2):
                strips = [ref[y ^ k, :, pl.ds(h * 288, 288)] for k in range(4)]
                rows = jnp.concatenate(strips, 1)
                for group in range(groups):
                    top = group * 128 + (h * 4 + (x_ref[0] ^ step)) * 16
                    part[pl.ds(pl.multiple_of(top, 16), 16), :] = rows[group * 16 : group * 16 + 16]
        shape = (COUNT * 4, COUNT * 4)
        to, come = iota(shape, 0), iota(shape, 1)
        swap = one_hot((come // 4 == spot(to // 4, own_ref[0])) & (come % 4 == to % 4))
        for group in range(groups if permuted else 0):
            at = pl.ds(group * 128, 128)
            moved = jnp.dot(swap, part[at, :], preferred_element_type=jnp.float32)
            part[at, :] = moved.astype(part.dtype)
        turned[...] = part[...].T

    firsts = []
    for ref in (low_ref, high_ref):
        first = jnp.dot(ref[...], turned[...], preferred_element_type=jnp.float32).T
        firsts.append(first.reshape(groups, COUNT, 4, block))
    firsts = jnp.concatenate(firsts, 2).astype(jnp.bfloat16)
    for group in range(groups):
        at = pl.ds(pl.multiple_of(group * HALF + pl.program_id(0) * block, 128), block)
        for step, ref in enumerate(near_refs):
            ref[:, :, at] = firsts[group, 8 * step : 8 * step + 8]
        for ref in far_refs:
            ref[:, :, at] = firsts[group]


def first_product(slabs, flat, own, x, permuted):
    block = 384
    steps = HALF // block
    groups = slabs[0].shape[1] // 16
    shapes = [(8, 8, groups * HALF)] * 4 if permuted else [(COUNT, 8, groups * HALF)]
    whole = lambda shape: pl.BlockSpec(shape, lambda i: (0,) * len(shape))
    shapes.append((groups * 128, NBASIS))
    return pl.pallas_call(
        functools.partial(first_kernel, groups=groups, permuted=permuted),
        grid=(steps,),
        in_specs=[pl.BlockSpec(memory_space=pltpu.SMEM)] * 2
        + [whole(slabs[0].shape)] * 4
        + [
            pl.BlockSpec((block, NBASIS), lambda i: (i, 0)),
            pl.BlockSpec((block, NBASIS), lambda i: (i + steps, 0)),
        ],
        out_specs=[whole(shape) for shape in shapes],
        out_shape=[jax.ShapeDtypeStruct(shape, jnp.bfloat16) for shape in shapes],
        scratch_shapes=[pltpu.VMEM((NBASIS, groups * 128), jnp.bfloat16)],
        compiler_params=pltpu.CompilerParams(vmem_limit_bytes=ALL_VMEM),
    )(own.reshape(1), x.reshape(1), *slabs, flat, flat)


def slot_of(r, j):
    tile, odd = r // 2, r % 2
    return jnp.where(
        tile < 16, odd * 512 + tile * 32 + j, 1024 + odd * 64 + (tile - 16) * 32 + j
    )


def second_kernel(got_ref, panel_ref, *rest):
    out_ref, wide, lhs = rest[-3:]
    size = COUNT * 8
    for tile in range(HALF // 128):
        piece = got_ref[:, :, pl.ds(tile * 128, 128)].astype(jnp.float32)
        wide[pl.ds(tile * size, size), :] = piece.reshape(size, 128)
    for l in range(4):
        rows = pl.ds(l * PAIRS, PAIRS)
        for start in range(0, 18, 4):
            parts = []
            for tile in range(start, min(start + 4, 18)):
                top = tile % 9 * size + tile // 9 * 4 + l
                parts.append(wide[pl.ds(top, COUNT, stride=8), :])
            turned = jnp.concatenate(parts, 0).astype(jnp.bfloat16).T
            if len(parts) == 4:
                lhs[rows, pl.ds(start * 32, 128)] = turned[:PAIRS]
                lhs[rows, pl.ds(512 + start * 32, 128)] = turned[PAIRS:]
            else:
                lhs[rows, pl.ds(1024, 128)] = jnp.concatenate([turned[:PAIRS], turned[PAIRS:]], 1)
    product = jnp.dot(lhs[...], panel_ref[...], preferred_element_type=jnp.float32)
    out_ref[...] = product.astype(out_ref.dtype).reshape(out_ref.shape)


def second(got, ordered, into, lo):
    specs = [
        pl.BlockSpec((COUNT, 8, HALF), lambda i: (0, 0, i)),
        pl.BlockSpec(ordered.shape, lambda i: (0, 0)),
    ]
    operands = [got, ordered]
    aliases = {}
    if into is not None:
        specs.append(pl.BlockSpec(memory_space=pl.ANY))
        operands.append(into)
        aliases = {2: 0}
    return pl.pallas_call(
        second_kernel,
        grid=(got.shape[2] // HALF,),
        in_specs=specs,
        out_specs=pl.BlockSpec((4, PAIRS, NORB), lambda i: (lo + i, 0, 0)),
        out_shape=jax.ShapeDtypeStruct((MINE, PAIRS, NORB), jnp.bfloat16),
        scratch_shapes=[
            pltpu.VMEM((COUNT * 8 * HALF // 128, 128), jnp.float32),
            pltpu.VMEM((4 * PAIRS, NBASIS), jnp.bfloat16),
        ],
        input_output_aliases=aliases,
        compiler_params=pltpu.CompilerParams(vmem_limit_bytes=ALL_VMEM),
        name="second",
    )(*operands)


def ordering(panel, place_of):
    shape = (NBASIS, NBASIS)
    slot = slot_of(iota(shape, 1) % ROWS, place_of(iota(shape, 1) // ROWS))
    return pick(one_hot(slot == iota(shape, 0)), panel)


def columns_of(first, groups, strip):
    shape = (16 * groups, WIDTH)
    row = iota(shape, 0)
    column = row % 16 // 4 * MINE + (first + row // 16) * 4 + row % 4
    chosen = one_hot(iota(shape, 1) == column)
    rows = jnp.dot(chosen, strip.reshape(-1, WIDTH).T, preferred_element_type=jnp.float32)
    return rows.astype(jnp.bfloat16)


def spread(first):
    held = [first[0]]
    for step in (1, 2, 3):
        held.append(lax.ppermute(first[step], "rs", [(j, j ^ step * 2) for j in range(COUNT)]))
    held = jnp.stack(held, 1)
    got = [held[0]]
    for step in range(1, 8):
        pairs = [(j, j ^ (step // 2 * 8 + step % 2)) for j in range(COUNT)]
        got.append(lax.ppermute(held[step], "rs", pairs))
    return jnp.concatenate(got, 0)


def on_device(integrals, coeff):
    x = lax.axis_index("pq") % 4
    own = lax.axis_index("rs")
    flat = integrals.transpose(1, 0, 2).reshape(LANES, NBASIS)

    strip = from_group(coeff, ALONG_Z).reshape(2, 8 * ROWS, WIDTH)

    def gathered(first, groups):
        columns = columns_of(first, groups, strip)
        slab = [columns]
        for step in (1, 2, 3):
            slab.append(lax.ppermute(columns, "rs", [(j, j ^ step * 8) for j in range(COUNT)]))
        slab = jnp.stack(slab)
        slabs = [slab]
        for step in (1, 2, 3):
            pairs = [(i, i & 4 | (i & 3) ^ step) for i in range(8)]
            slabs.append(lax.ppermute(slab, "pq", pairs))
        return slabs

    early = gathered(0, SOON)
    late = gathered(SOON, FAR)
    *soon, soon_part = first_product(early, flat, own, x, True)
    far, far_part = first_product(late, flat, own, x, False)

    got_soon = spread(soon)
    got_far = lax.all_to_all(far, "rs", 0, 0, tiled=True)

    far_part, mine = lax.optimization_barrier((far_part, own))
    parts = jnp.concatenate([soon_part, far_part], 0)
    g = iota((NORB, NORB), 0)
    d = g % 128 // 4
    j = jnp.where(g < SOON * 128, spot(d, mine), d)
    put = one_hot(iota((NORB, NORB), 1) == j * MINE + g // 128 * 4 + g % 4)
    panel = jnp.einsum("gs,gk->sk", parts, put, preferred_element_type=jnp.float32)
    panel = panel.astype(jnp.bfloat16)
    ordered = ordering(panel, lambda j: j)
    crossed = ordering(
        panel, lambda j: ((j ^ mine) & 24) | ((j ^ mine) & 1) << 2 | ((j ^ mine) & 6) >> 1
    )
    out = second(got_soon, crossed, None, 0)
    out = second(got_far, ordered, out, SOON)
    return out.transpose(1, 0, 2)


def solution(mesh):
    placed = (P("pq", "rs", None), P("rs", "pq"))
    return jax.shard_map(
        on_device, mesh=mesh, in_specs=placed, out_specs=P("pq", "rs", None), check_vma=False
    )
```
